32 devices in a mesh: col: 16 (over z, y, x), lev: 2 (over core).
Axes of the slice: x: 2, y: 2, z: 4, core: 2. Of those that a mesh axis runs over, the one named last changes fastest.
Arguments:
- perturbations: float32 [80, 16, 16384], P(None, 'lev', 'col'), may hold values from -0.625 to 0.625
- gradient: float32 [32, 16, 16384], P(None, 'lev', 'col'), may hold values from -2 to 2
- horizontal: float32 [20, 16384], P(None, 'col'), may hold values from -50 to 50
- area: float32 [16384], P('col'), may hold values from 1 to 60
- vertical: float32 [20, 16], P(None, 'lev'), may hold values from -1.25 to 1.25
Outputs:
- increment: float32 [32, 16, 16384], P(None, 'lev', 'col')
- background: float32 [32], replicated
The draws below stay inside these ranges and needn't reach their ends.
All inputs are finite; a program needn't handle non-finite values.
Results may differ from the reference program's by a relative error of at most 0.0003.
Values sent between devices are 32-bit elements; how exact they have to be, the bound alone decides.
No kernel may reach another device: no remote copies, remote signals or barrier semaphores. Data moves between devices by JAX's collectives and lax.ppermute only.
A program may use at most 128 MiB of HBM per device.

```python
import math
import jax
import jax.numpy as jnp
from jax import lax

MEMBERS = 80
VMODES = 20
HMODES = 20
VECTORS = 32
LEV = 16
COLS = 16384


def draw_area(key, part):
    position = jnp.arange(COLS).astype(jnp.float32)
    ramped = 1.0 + 2.0 * position / max(COLS - 1, 1)
    rough = jnp.exp(jax.random.uniform(key, (COLS,), jnp.float32, 0.0, math.log(10.0)))
    return ramped * rough


def draw_horizontal(key, part):
    first, second = jax.random.split(jax.random.fold_in(key, 17), 2)
    row_scale = jnp.exp(jax.random.uniform(first, (HMODES, 1), jnp.float32, 0.0, math.log(10.0)))
    column_values = jnp.clip(jax.random.normal(second, (HMODES, COLS), jnp.float32), -5.0, 5.0)
    return row_scale * column_values


def shard_levels(key, dims, cuts, least, top_value):
    def one(dim, blocks):
        draws = jax.random.uniform(jax.random.fold_in(jax.random.fold_in(key, 6), dim), (blocks,), jnp.float32, least / len(cuts), top_value / len(cuts))
        return jnp.repeat(jnp.exp(draws), dims[dim] // blocks).reshape((-1,) + (1,) * (len(dims) - dim - 1))

    factor_of = one(*cuts[0])
    for cut in cuts[1:]:
        factor_of = factor_of * one(*cut)
    return factor_of


def centred(key, extent, width, bound, shards=(), dtype=jnp.bfloat16):
    values = width * jax.random.normal(key, extent, jnp.float32)
    if shards:
        values = values * shard_levels(key, extent, shards, -0.22, 0.18)
    return jnp.clip(values, -bound, bound).astype(dtype)


def setup_inputs(seed: int = 0) -> dict:
    seeds = jax.random.split(jax.random.key(seed), 6)
    return {
        "perturbations": centred(seeds[0], (MEMBERS, LEV, COLS), MEMBERS ** -0.5, 0.625, ((1, 2), (2, 16)), jnp.float32),
        "gradient": centred(seeds[1], (VECTORS, LEV, COLS), (max(1, LEV * COLS // (VMODES * HMODES * MEMBERS))) ** -0.5, 2.0, ((1, 2), (2, 16)), jnp.float32),
        "horizontal": draw_horizontal(jax.random.fold_in(seeds[5], 71), 0),
        "area": draw_area(jax.random.fold_in(seeds[5], 71), 0),
        "vertical": centred(seeds[4], (VMODES, LEV), VMODES ** -0.5, 1.25, ((1, 2),), jnp.float32),
    }


TOP_PRECISION = lax.Precision.HIGHEST

def reference(perturbations, gradient, horizontal, area, vertical):
    area_sum = jnp.sum(area)
    mode_power = lax.optimization_barrier(jnp.sum(area[None, :] * horizontal * horizontal, axis=1))
    scaled_terms = horizontal / jnp.sqrt(HMODES * (mode_power / area_sum + 1e-06))[:, None]
    weight = area * (COLS / area_sum)

    def adjoint_level(level_index):
        level_index = level_index.astype(jnp.int32)
        ensemble_member_rows = lax.dynamic_index_in_dim(perturbations, level_index, 1, keepdims=False)
        gradient_rows = lax.dynamic_index_in_dim(gradient, level_index, 1, keepdims=False)
        mode_products = (gradient_rows * weight[None, :])[:, None, :] * scaled_terms[None, :, :]
        return jnp.einsum('kc,vbc->kvb', ensemble_member_rows, mode_products, precision=TOP_PRECISION)
    terms = lax.map(adjoint_level, jnp.arange(LEV).astype(jnp.int32))
    control = jnp.einsum('al,lkvb->vkab', vertical, terms, precision=TOP_PRECISION)
    lifted = jnp.einsum('al,vkab->lkvb', vertical, control, precision=TOP_PRECISION)

    def forward_level_map(level_index):
        level_index = level_index.astype(jnp.int32)
        ensemble_member_rows = lax.dynamic_index_in_dim(perturbations, level_index, 1, keepdims=False)
        level_lift = lax.dynamic_index_in_dim(lifted, level_index, 0, keepdims=False)
        member_spread = jnp.einsum('kvb,kc->vbc', level_lift, ensemble_member_rows, precision=TOP_PRECISION)
        return lax.optimization_barrier(jnp.sum(member_spread * scaled_terms[None, :, :], axis=1))
    by_level = lax.map(forward_level_map, jnp.arange(LEV).astype(jnp.int32))
    increment = jnp.transpose(by_level, (1, 0, 2))
    background = 0.5 * lax.optimization_barrier(jnp.sum(control * control, axis=(1, 2, 3)))
    return (increment, background)
```

```python
import functools

import jax
import jax.numpy as jnp
from jax import lax
from jax.experimental import pallas as pl
from jax.experimental.pallas import tpu as pltpu
from jax.sharding import Mesh, PartitionSpec as P

LANES = 128
SUBLANES = 8


def split(x):
    high = x.astype(jnp.bfloat16)
    return high, (x - high.astype(jnp.float32)).astype(jnp.bfloat16)


def dot(a, b, dims):
    return lax.dot_general(a, b, (dims, ((), ())), preferred_element_type=jnp.float32)


def spread_lanes(ref, strips):
    rows = ref.shape[0]
    for j in range(ref.shape[1] // LANES):
        strips[j * rows : (j + 1) * rows, :] = ref[:, j * LANES : (j + 1) * LANES]


def level_rows(strips, rows, strip_count, level, levels):
    count = rows // levels
    return jnp.concatenate(
        [strips[pl.ds(j * rows + level, count, stride=levels), :] for j in range(strip_count)],
        axis=1,
    )


def adjoint_kernel(p_ref, g_ref, h_ref, area_ref, out_ref, terms, ps, gs, *, sizes):
    members, levels, vectors, modes, share, parts = sizes
    level = pl.program_id(0)
    units_a_row = modes * vectors // LANES
    area = area_ref[...]
    strips = p_ref.shape[1] // LANES

    @pl.when(level == 0)
    def _():
        spread_lanes(p_ref, ps)
        spread_lanes(g_ref, gs)

    p = level_rows(ps, members * levels, strips, level, levels)
    g = level_rows(gs, vectors * levels, strips, level, levels) * area
    p_high, p_low = split(p)
    both = jnp.concatenate([p_high, p_low], axis=0)
    group = LANES // vectors
    for q in range(units_a_row):
        mode_products = jnp.concatenate(
            [g * h_ref[q * group + i : q * group + i + 1, :] for i in range(group)], axis=0
        )
        high, low = split(mode_products)
        first = dot(both, high, ((1,), (1,)))
        second = dot(p_high, low, ((1,), (1,)))
        sums = first[:members] + (first[members:] + second)
        terms[pl.ds(q * levels + level, members, stride=units_a_row * levels), :] = sums

    @pl.when(level == pl.num_programs(0) - 1)
    def _():
        total = members * units_a_row
        h = h_ref[...]
        power = jnp.sum(area * h * h, axis=1, keepdims=True)
        rows = -(-(modes + 1) // SUBLANES) * SUBLANES
        area_sum = jnp.sum(area, axis=1, keepdims=True)
        stats = jnp.concatenate(
            [power, area_sum, jnp.zeros((rows - modes - 1, 1), jnp.float32)], axis=0
        )
        stats = jnp.broadcast_to(stats, (rows, LANES))
        lane = lax.broadcasted_iota(jnp.int32, (rows, LANES), 1)
        row = lax.broadcasted_iota(jnp.int32, (rows, LANES), 0)
        stats = jnp.sum(jnp.where(lane == row, stats, 0.0), axis=0, keepdims=True)
        stats = jnp.broadcast_to(stats, (levels, LANES))
        width = (share + 1) * levels
        for part in range(parts):
            begin = min(part * share, total)
            end = min(begin + share, total)
            filled = part * width + (end - begin) * levels
            if end > begin:
                out_ref[part * width : filled, :] = terms[begin * levels : end * levels, :]
            if end - begin < share:
                rest = (part + 1) * width - levels - filled
                out_ref[filled : filled + rest, :] = jnp.zeros((rest, LANES), jnp.float32)
            out_ref[(part + 1) * width - levels : (part + 1) * width, :] = stats


def forward_kernel(l_ref, p_ref, h_ref, factor_ref, out_ref, terms, ps, os, *, sizes):
    members, levels, vectors, modes, share, parts = sizes
    level = pl.program_id(0)
    units_a_row = modes * vectors // LANES
    total = members * units_a_row

    @pl.when(level == 0)
    def _():
        spread_lanes(p_ref, ps)
        width = (share + 1) * levels
        for part in range(parts):
            begin, end = part * share, min((part + 1) * share, total)
            if end > begin:
                terms[begin * levels : end * levels, :] = l_ref[
                    part * width : part * width + (end - begin) * levels, :
                ]

    strips = p_ref.shape[1] // LANES
    p = level_rows(ps, members * levels, strips, level, levels)
    p_high, p_low = split(p)
    right = jnp.concatenate([p_high, p_low, p_high], axis=0)
    group = LANES // vectors
    acc = None
    for q in range(units_a_row):
        lifted = terms[pl.ds(q * levels + level, members, stride=units_a_row * levels), :]
        high, low = split(lifted)
        left = jnp.concatenate([high, high, low], axis=0)
        spread = dot(left, right, ((0,), (0,)))
        for i in range(group):
            b = q * group + i
            scaled = h_ref[b : b + 1, :] * factor_ref[b : b + 1, :]
            piece = spread[i * vectors : (i + 1) * vectors] * scaled
            acc = piece if acc is None else acc + piece
    rows = vectors * levels
    for j in range(strips):
        os[pl.ds(j * rows + level, vectors, stride=levels), :] = acc[:, j * LANES : (j + 1) * LANES]

    @pl.when(level == pl.num_programs(0) - 1)
    def _():
        for j in range(strips):
            out_ref[:, j * LANES : (j + 1) * LANES] = os[j * rows : (j + 1) * rows, :]


def exchange(blocks, axis):
    return lax.all_to_all(blocks, axis, 0, 0, tiled=True)


def per_device(perturbations, gradient, horizontal, area, vertical, *, inner, outer, lev):
    members, levels, columns = perturbations.shape
    vectors = gradient.shape[0]
    modes = horizontal.shape[0]
    units_a_row = modes * vectors // LANES
    total = members * units_a_row
    parts = inner * outer * lev
    share = -(-total // parts)
    sizes = (members, levels, vectors, modes, share, parts)
    p2 = perturbations.reshape(members * levels, columns)
    g2 = gradient.reshape(vectors * levels, columns)
    whole = lambda *shape: pl.BlockSpec(shape, lambda l: (0,) * len(shape))
    rows = parts * (share + 1) * levels
    params = pltpu.CompilerParams(
        dimension_semantics=("arbitrary",), vmem_limit_bytes=48 * 1024 * 1024
    )
    sent = pl.pallas_call(
        functools.partial(adjoint_kernel, sizes=sizes),
        grid=(levels,),
        in_specs=[
            whole(members * levels, columns),
            whole(vectors * levels, columns),
            whole(modes, columns),
            whole(1, columns),
        ],
        out_specs=whole(rows, LANES),
        out_shape=jax.ShapeDtypeStruct((rows, LANES), jnp.float32),
        scratch_shapes=[
            pltpu.VMEM((total * levels, LANES), jnp.float32),
            pltpu.VMEM((members * levels * columns // LANES, LANES), jnp.float32),
            pltpu.VMEM((vectors * levels * columns // LANES, LANES), jnp.float32),
        ],
        compiler_params=params,
        name="adjoint",
    )(p2, g2, horizontal, area[None, :])

    unit = share + 1
    got = exchange(sent.reshape(inner, -1, LANES), "ci").sum(0)
    got = exchange(got.reshape(outer * lev, unit, levels, LANES), ("co", "lev"))
    got = got.reshape(outer, lev, unit, levels, LANES).sum(0)
    stats = got[0, -1, 0]
    area_sum = stats[modes]
    factor = 1.0 / jnp.sqrt(modes * (stats[:modes] / area_sum + 1e-06))
    scale = columns * inner * outer / area_sum
    vertical_all = lax.all_gather(vertical, "lev", axis=0)
    control = jnp.einsum(
        "mal,muln->aun",
        vertical_all, got[:, :-1], precision=lax.Precision.HIGHEST,
    )
    lifted = jnp.einsum(
        "mal,aun->muln", vertical_all, control, precision=lax.Precision.HIGHEST
    )
    index = (lax.axis_index("ci") * outer + lax.axis_index("co")) * lev + lax.axis_index("lev")
    squares = jnp.sum(control * control, axis=0)
    place = (index * share + jnp.arange(share)) % units_a_row
    mine = (place[:, None] == jnp.arange(levels)[None, :]).astype(jnp.float32)
    rows_q = jnp.sum(mine[:, :, None] * squares[:, None, :], axis=0)
    back = jnp.concatenate(
        [lifted, jnp.broadcast_to(rows_q[None, None], (lev, 1, levels, LANES))], axis=1
    )
    back = jnp.broadcast_to(back[None], (outer,) + back.shape)
    back = exchange(back.reshape(outer * lev, unit * levels, LANES), ("co", "lev"))
    back = back.reshape(1, -1, LANES)
    back = exchange(jnp.broadcast_to(back, (inner,) + back.shape[1:]), "ci")
    back = back.reshape(rows, LANES)
    squares_all = jnp.sum(back.reshape(parts, unit, levels, LANES)[:, -1], axis=0)
    by_mode = squares_all[:units_a_row].reshape(modes, vectors)
    whole_factor = factor * scale
    background = 0.5 * jnp.sum(by_mode * (whole_factor * whole_factor)[:, None], axis=0)
    factor_rows = jnp.broadcast_to((factor * whole_factor)[:, None], (modes, columns))
    increment = pl.pallas_call(
        functools.partial(forward_kernel, sizes=sizes),
        grid=(levels,),
        in_specs=[
            whole(rows, LANES),
            whole(members * levels, columns),
            whole(modes, columns),
            whole(modes, columns),
        ],
        out_specs=whole(vectors * levels, columns),
        out_shape=jax.ShapeDtypeStruct((vectors * levels, columns), jnp.float32),
        scratch_shapes=[
            pltpu.VMEM((total * levels, LANES), jnp.float32),
            pltpu.VMEM((members * levels * columns // LANES, LANES), jnp.float32),
            pltpu.VMEM((vectors * levels * columns // LANES, LANES), jnp.float32),
        ],
        compiler_params=params,
        name="forward",
    )(back, p2, horizontal, factor_rows)
    return increment.reshape(vectors, levels, columns), background


def solution(mesh):
    count, lev = mesh.shape["col"], mesh.shape["lev"]
    inner = 4 if count % 4 == 0 else 1
    outer = count // inner
    split_mesh = Mesh(mesh.devices.reshape(outer, inner, lev), ("co", "ci", "lev"))
    col = ("co", "ci")
    return jax.shard_map(
        functools.partial(per_device, inner=inner, outer=outer, lev=lev),
        mesh=split_mesh,
        in_specs=(
            P(None, "lev", col),
            P(None, "lev", col),
            P(None, col),
            P(col),
            P(None, "lev"),
        ),
        out_specs=(P(None, "lev", col), P()),
        check_vma=False,
    )
```

```python
import functools

import jax
import jax.numpy as jnp
from jax import lax
from jax.experimental import pallas as pl
from jax.experimental.pallas import tpu as pltpu
from jax.sharding import Mesh, PartitionSpec as P

LANES = 128
SUBLANES = 8


def split(x):
    high = x.astype(jnp.bfloat16)
    return high, (x - high.astype(jnp.float32)).astype(jnp.bfloat16)


def dot(a, b, dims):
    return lax.dot_general(a, b, (dims, ((), ())), preferred_element_type=jnp.float32)


def spread_lanes(ref, strips):
    rows = ref.shape[0]
    for j in range(ref.shape[1] // LANES):
        strips[j * rows : (j + 1) * rows, :] = ref[:, j * LANES : (j + 1) * LANES]


def level_rows(strips, rows, strip_count, level, levels):
    count = rows // levels
    return jnp.concatenate(
        [strips[pl.ds(j * rows + level, count, stride=levels), :] for j in range(strip_count)],
        axis=1,
    )


def adjoint_kernel(where, p_ref, g_ref, h_ref, area_ref, *rest, sizes, piece):
    members, levels, vectors, modes, inner, others = sizes
    first_q, count_q, share, extra = piece
    outs, (terms, ps, gs) = rest[:inner], rest[inner:]
    level = pl.program_id(0)
    area = area_ref[...]
    strips = p_ref.shape[1] // LANES
    total = members * count_q

    @pl.when(level == 0)
    def _():
        spread_lanes(p_ref, ps)
        spread_lanes(g_ref, gs)
        pad = inner * others * share - total
        if pad:
            terms[total * levels :, :] = jnp.zeros((pad * levels, LANES), jnp.float32)

    p = level_rows(ps, members * levels, strips, level, levels)
    g = level_rows(gs, vectors * levels, strips, level, levels) * area
    p_high, p_low = split(p)
    both = jnp.concatenate([p_high, p_low], axis=0)
    group = LANES // vectors
    for q in range(count_q):
        start = (first_q + q) * group
        mode_products = jnp.concatenate(
            [g * h_ref[start + i : start + i + 1, :] for i in range(group)], axis=0
        )
        high, low = split(mode_products)
        first = dot(both, high, ((1,), (1,)))
        second = dot(p_high, low, ((1,), (1,)))
        sums = first[:members] + (first[members:] + second)
        terms[pl.ds(q * levels + level, members, stride=count_q * levels), :] = sums

    @pl.when(level == pl.num_programs(0) - 1)
    def _():
        if extra:
            h = h_ref[...]
            power = jnp.sum(area * h * h, axis=1, keepdims=True)
            rows = -(-(modes + 1) // SUBLANES) * SUBLANES
            area_sum = jnp.sum(area, axis=1, keepdims=True)
            stats = jnp.concatenate(
                [power, area_sum, jnp.zeros((rows - modes - 1, 1), jnp.float32)], axis=0
            )
            stats = jnp.broadcast_to(stats, (rows, LANES))
            lane = lax.broadcasted_iota(jnp.int32, (rows, LANES), 1)
            row = lax.broadcasted_iota(jnp.int32, (rows, LANES), 0)
            stats = jnp.sum(jnp.where(lane == row, stats, 0.0), axis=0, keepdims=True)
            stats = jnp.broadcast_to(stats, (levels, LANES))
        width = (share + extra) * levels
        used = share * levels
        for s in range(inner):
            for t in range(others):
                part = (where[0] ^ s) * others + (where[1] ^ t)
                outs[s][t * width : t * width + used, :] = terms[pl.ds(part * used, used), :]
                if extra:
                    outs[s][t * width + used : (t + 1) * width, :] = stats


def forward_kernel(where, p_ref, h_ref, factor_ref, *rest, sizes, piece, added):
    members, levels, vectors, modes, inner, others = sizes
    first_q, count_q, share, extra = piece
    lifts = rest[:inner]
    rest = rest[inner:]
    base_ref = rest[0] if added else None
    out_ref, terms, ps, os = rest[1:] if added else rest
    level = pl.program_id(0)
    strips = p_ref.shape[1] // LANES
    rows = vectors * levels

    @pl.when(level == 0)
    def _():
        spread_lanes(p_ref, ps)
        width = (share + extra) * levels
        used = share * levels
        for s in range(inner):
            for t in range(others):
                part = (where[0] ^ s) * others + (where[1] ^ t)
                terms[pl.ds(part * used, used), :] = lifts[s][t * width : t * width + used, :]

    p = level_rows(ps, members * levels, strips, level, levels)
    p_high, p_low = split(p)
    right = jnp.concatenate([p_high, p_low, p_high], axis=0)
    group = LANES // vectors
    acc = None
    for q in range(count_q):
        lifted = terms[pl.ds(q * levels + level, members, stride=count_q * levels), :]
        high, low = split(lifted)
        left = jnp.concatenate([high, high, low], axis=0)
        spread = dot(left, right, ((0,), (0,)))
        for i in range(group):
            b = (first_q + q) * group + i
            scaled = h_ref[b : b + 1, :] * factor_ref[b : b + 1, :]
            product = spread[i * vectors : (i + 1) * vectors] * scaled
            acc = product if acc is None else acc + product
    for j in range(strips):
        os[pl.ds(j * rows + level, vectors, stride=levels), :] = acc[:, j * LANES : (j + 1) * LANES]

    @pl.when(level == pl.num_programs(0) - 1)
    def _():
        for j in range(strips):
            lanes = slice(j * LANES, (j + 1) * LANES)
            made = os[j * rows : (j + 1) * rows, :]
            out_ref[:, lanes] = made + base_ref[:, lanes] if added else made


def send(block, axis, size, step):
    return lax.ppermute(block, axis, [(j, j ^ step) for j in range(size)])


def pieces_of(rows, parts, members):
    cut = (rows * 2) // 5
    bounds = [(0, cut), (cut, rows)] if cut else [(0, rows)]
    return [(a, b - a, -(-members * (b - a) // parts)) for a, b in bounds]


def per_device(perturbations, gradient, horizontal, area, vertical, *, inner, outer, lev):
    members, levels, columns = perturbations.shape
    vectors = gradient.shape[0]
    modes = horizontal.shape[0]
    others = outer * lev
    parts = inner * others
    sizes = (members, levels, vectors, modes, inner, others)
    p2 = perturbations.reshape(members * levels, columns)
    g2 = gradient.reshape(vectors * levels, columns)
    area2 = area[None, :]
    ci = lax.axis_index("ci")
    rest = lax.axis_index("co") * lev + lax.axis_index("lev")
    where = jnp.stack([ci, rest]).astype(jnp.int32)
    units_a_row = modes * vectors // LANES
    pieces = pieces_of(units_a_row, parts, members)
    whole = lambda *shape: pl.BlockSpec(shape, lambda l, w: (0,) * len(shape))
    params = pltpu.CompilerParams(
        dimension_semantics=("arbitrary",), vmem_limit_bytes=40 * 1024 * 1024
    )
    strips_shape = pltpu.VMEM((members * levels * columns // LANES, LANES), jnp.float32)
    rows_shape = pltpu.VMEM((vectors * levels * columns // LANES, LANES), jnp.float32)
    everywhere = ("co", "lev")

    vertical_of = [
        vertical if m == 0 else send(vertical, "lev", lev, m) for m in range(lev)
    ]
    precise = dict(precision=lax.Precision.HIGHEST)

    received = []
    for n, (first_q, count_q, share) in enumerate(pieces):
        extra = 1 if n == 0 else 0
        width = (share + extra) * levels
        outs = pl.pallas_call(
            functools.partial(
                adjoint_kernel, sizes=sizes, piece=(first_q, count_q, share, extra)
            ),
            grid_spec=pltpu.PrefetchScalarGridSpec(
                num_scalar_prefetch=1,
                grid=(levels,),
                in_specs=[
                    whole(members * levels, columns),
                    whole(vectors * levels, columns),
                    whole(modes, columns),
                    whole(1, columns),
                ],
                out_specs=[whole(others * width, LANES)] * inner,
                scratch_shapes=[
                    pltpu.VMEM((parts * share * levels, LANES), jnp.float32),
                    strips_shape,
                    rows_shape,
                ],
            ),
            out_shape=[jax.ShapeDtypeStruct((others * width, LANES), jnp.float32)] * inner,
            compiler_params=params,
            name=f"adjoint_{n}",
        )(where, p2, g2, horizontal, area2)
        received.append([outs[0]] + [send(outs[s], "ci", inner, s) for s in range(1, inner)])

    arrived = []
    for (first_q, count_q, share), blocks in zip(pieces, received):
        width = blocks[0].shape[0] // others
        slots = []
        for t in range(others):
            cut = slice(t * width, (t + 1) * width)
            slot = functools.reduce(lambda a, b: a + b, [block[cut] for block in blocks])
            slots.append(send(slot, everywhere, others, t) if t else slot)
        arrived.append(slots)

    squares_rows = jnp.zeros((levels, LANES), jnp.float32)
    lifts = []
    for n, ((first_q, count_q, share), slots) in enumerate(zip(pieces, arrived)):
        sums = [
            functools.reduce(lambda a, b: a + b, slots[m::lev]).reshape(-1, levels, LANES)
            for m in range(lev)
        ]
        if n == 0:
            stats = sums[0][-1, 0]
        control = sum(
            jnp.einsum("al,uln->aun", vertical_of[m], sums[m][:share], **precise)
            for m in range(lev)
        )
        squares = jnp.sum(control * control, axis=0)
        place = first_q + ((ci * others + rest) * share + jnp.arange(share)) % count_q
        mine = (place[:, None] == jnp.arange(levels)[None, :])[:, :, None]
        squares_rows = squares_rows + jnp.sum(jnp.where(mine, squares[:, None, :], 0.0), axis=0)
        last = n == len(pieces) - 1
        lifted = []
        for m in range(lev):
            made = jnp.einsum("al,aun->uln", vertical_of[m], control, **precise)
            if last:
                made = jnp.concatenate([made, squares_rows[None]], axis=0)
            lifted.append(made.reshape(-1, LANES))
        block = jnp.concatenate(
            [lifted[t % lev] if t == 0 else send(lifted[t % lev], everywhere, others, t) for t in range(others)],
            axis=0,
        )
        lifts.append([block] + [send(block, "ci", inner, s) for s in range(1, inner)])

    area_sum = stats[modes]
    factor = 1.0 / jnp.sqrt(modes * (stats[:modes] / area_sum + 1e-06))
    whole_factor = factor * (columns * inner * outer / area_sum)
    factor_rows = jnp.broadcast_to((factor * whole_factor)[:, None], (modes, columns))

    increment = None
    for n, ((first_q, count_q, share), blocks) in enumerate(zip(pieces, lifts)):
        extra = 1 if n == len(pieces) - 1 else 0
        width = (share + extra) * levels
        added = increment is not None
        increment = pl.pallas_call(
            functools.partial(
                forward_kernel, sizes=sizes, piece=(first_q, count_q, share, extra), added=added
            ),
            grid_spec=pltpu.PrefetchScalarGridSpec(
                num_scalar_prefetch=1,
                grid=(levels,),
                in_specs=[
                    whole(members * levels, columns),
                    whole(modes, columns),
                    whole(modes, columns),
                ]
                + [whole(others * width, LANES)] * inner
                + ([whole(vectors * levels, columns)] if added else []),
                out_specs=whole(vectors * levels, columns),
                scratch_shapes=[
                    pltpu.VMEM((parts * share * levels, LANES), jnp.float32),
                    strips_shape,
                    rows_shape,
                ],
            ),
            out_shape=jax.ShapeDtypeStruct((vectors * levels, columns), jnp.float32),
            compiler_params=params,
            name=f"forward_{n}",
        )(where, p2, horizontal, factor_rows, *blocks, *([increment] if added else []))

    squares_all = sum(
        jnp.sum(block.reshape(others, -1, levels, LANES)[:, -1], axis=0) for block in lifts[-1]
    )
    by_mode = squares_all[:units_a_row].reshape(modes, vectors)
    background = 0.5 * jnp.sum(by_mode * (whole_factor * whole_factor)[:, None], axis=0)
    return increment.reshape(vectors, levels, columns), background


def solution(mesh):
    count, lev = mesh.shape["col"], mesh.shape["lev"]
    inner = 4
    outer = count // inner
    split_mesh = Mesh(mesh.devices.reshape(outer, inner, lev), ("co", "ci", "lev"))
    col = ("co", "ci")
    return jax.shard_map(
        functools.partial(per_device, inner=inner, outer=outer, lev=lev),
        mesh=split_mesh,
        in_specs=(
            P(None, "lev", col),
            P(None, "lev", col),
            P(None, col),
            P(col),
            P(None, "lev"),
        ),
        out_specs=(P(None, "lev", col), P()),
        check_vma=False,
    )
```

```python
import functools

import jax
import jax.numpy as jnp
from jax import lax
from jax.experimental import pallas as pl
from jax.experimental.pallas import tpu as pltpu
from jax.sharding import Mesh, PartitionSpec as P

LANES = 128
SUBLANES = 8


def split(x):
    high = x.astype(jnp.bfloat16)
    return high, (x - high.astype(jnp.float32)).astype(jnp.bfloat16)


def dot(a, b, dims):
    return lax.dot_general(a, b, (dims, ((), ())), preferred_element_type=jnp.float32)


def spread_lanes(ref, strips):
    rows = ref.shape[0]
    for j in range(ref.shape[1] // LANES):
        strips[j * rows : (j + 1) * rows, :] = ref[:, j * LANES : (j + 1) * LANES]


def level_rows(strips, rows, strip_count, level, levels):
    count = rows // levels
    return jnp.concatenate(
        [strips[pl.ds(j * rows + level, count, stride=levels), :] for j in range(strip_count)],
        axis=1,
    )


def adjoint_kernel(where, p_ref, g_ref, h_ref, area_ref, *rest, sizes, piece):
    members, levels, vectors, modes, inner, others = sizes
    first_q, count_q, share, extra = piece
    outs, (terms, ps, gs) = rest[:inner], rest[inner:]
    level = pl.program_id(0)
    area = area_ref[...]
    strips = p_ref.shape[1] // LANES
    total = members * count_q

    @pl.when(level == 0)
    def _():
        spread_lanes(p_ref, ps)
        spread_lanes(g_ref, gs)
        pad = inner * others * share - total
        if pad:
            terms[total * levels :, :] = jnp.zeros((pad * levels, LANES), jnp.float32)

    p = level_rows(ps, members * levels, strips, level, levels)
    g = level_rows(gs, vectors * levels, strips, level, levels) * area
    p_high, p_low = split(p)
    both = jnp.concatenate([p_high, p_low], axis=0)
    group = LANES // vectors
    for q in range(count_q):
        start = (first_q + q) * group
        mode_products = jnp.concatenate(
            [g * h_ref[start + i : start + i + 1, :] for i in range(group)], axis=0
        )
        high, low = split(mode_products)
        first = dot(both, high, ((1,), (1,)))
        second = dot(p_high, low, ((1,), (1,)))
        sums = first[:members] + (first[members:] + second)
        terms[pl.ds(q * levels + level, members, stride=count_q * levels), :] = sums

    @pl.when(level == pl.num_programs(0) - 1)
    def _():
        if extra:
            h = h_ref[...]
            power = jnp.sum(area * h * h, axis=1, keepdims=True)
            rows = -(-(modes + 1) // SUBLANES) * SUBLANES
            area_sum = jnp.sum(area, axis=1, keepdims=True)
            stats = jnp.concatenate(
                [power, area_sum, jnp.zeros((rows - modes - 1, 1), jnp.float32)], axis=0
            )
            stats = jnp.broadcast_to(stats, (rows, LANES))
            lane = lax.broadcasted_iota(jnp.int32, (rows, LANES), 1)
            row = lax.broadcasted_iota(jnp.int32, (rows, LANES), 0)
            stats = jnp.sum(jnp.where(lane == row, stats, 0.0), axis=0, keepdims=True)
            stats = jnp.broadcast_to(stats, (levels, LANES))
        width = (share + extra) * levels
        used = share * levels
        for s in range(inner):
            for t in range(others):
                part = (where[0] ^ s) * others + t
                outs[s][t * width : t * width + used, :] = terms[pl.ds(part * used, used), :]
                if extra:
                    outs[s][t * width + used : (t + 1) * width, :] = stats


def forward_kernel(where, p_ref, h_ref, factor_ref, *rest, sizes, piece, added):
    members, levels, vectors, modes, inner, others = sizes
    first_q, count_q, share, extra = piece
    lifts = rest[:inner]
    rest = rest[inner:]
    base_ref = rest[0] if added else None
    out_ref, terms, ps, os = rest[1:] if added else rest
    level = pl.program_id(0)
    strips = p_ref.shape[1] // LANES
    rows = vectors * levels

    @pl.when(level == 0)
    def _():
        spread_lanes(p_ref, ps)
        width = (share + extra) * levels
        used = share * levels
        for s in range(inner):
            for t in range(others):
                part = (where[0] ^ s) * others + t
                terms[pl.ds(part * used, used), :] = lifts[s][t * width : t * width + used, :]

    p = level_rows(ps, members * levels, strips, level, levels)
    p_high, p_low = split(p)
    right = jnp.concatenate([p_high, p_low, p_high], axis=0)
    group = LANES // vectors
    acc = None
    for q in range(count_q):
        lifted = terms[pl.ds(q * levels + level, members, stride=count_q * levels), :]
        high, low = split(lifted)
        left = jnp.concatenate([high, high, low], axis=0)
        spread = dot(left, right, ((0,), (0,)))
        for i in range(group):
            b = (first_q + q) * group + i
            scaled = h_ref[b : b + 1, :] * factor_ref[b : b + 1, :]
            product = spread[i * vectors : (i + 1) * vectors] * scaled
            acc = product if acc is None else acc + product
    for j in range(strips):
        os[pl.ds(j * rows + level, vectors, stride=levels), :] = acc[:, j * LANES : (j + 1) * LANES]

    @pl.when(level == pl.num_programs(0) - 1)
    def _():
        for j in range(strips):
            lanes = slice(j * LANES, (j + 1) * LANES)
            made = os[j * rows : (j + 1) * rows, :]
            out_ref[:, lanes] = made + base_ref[:, lanes] if added else made


def send(block, axis, size, step):
    return lax.ppermute(block, axis, [(j, j ^ step) for j in range(size)])


def pieces_of(rows, parts, members):
    cut = (rows * 2) // 5
    bounds = [(0, cut), (cut, rows)] if cut else [(0, rows)]
    return [(a, b - a, -(-members * (b - a) // parts)) for a, b in bounds]


def per_device(perturbations, gradient, horizontal, area, vertical, *, inner, outer, lev):
    members, levels, columns = perturbations.shape
    vectors = gradient.shape[0]
    modes = horizontal.shape[0]
    others = outer * lev
    parts = inner * others
    sizes = (members, levels, vectors, modes, inner, others)
    p2 = perturbations.reshape(members * levels, columns)
    g2 = gradient.reshape(vectors * levels, columns)
    area2 = area[None, :]
    ci = lax.axis_index("ci")
    rest = lax.axis_index("co") * lev + lax.axis_index("lev")
    where = jnp.stack([ci, rest]).astype(jnp.int32)
    units_a_row = modes * vectors // LANES
    pieces = pieces_of(units_a_row, parts, members)
    whole = lambda *shape: pl.BlockSpec(shape, lambda l, w: (0,) * len(shape))
    params = pltpu.CompilerParams(
        dimension_semantics=("arbitrary",), vmem_limit_bytes=40 * 1024 * 1024
    )
    strips_shape = pltpu.VMEM((members * levels * columns // LANES, LANES), jnp.float32)
    rows_shape = pltpu.VMEM((vectors * levels * columns // LANES, LANES), jnp.float32)
    everywhere = ("co", "lev")

    vertical_all = lax.all_gather(vertical, "lev", axis=0)
    precise = dict(precision=lax.Precision.HIGHEST)

    received = []
    for n, (first_q, count_q, share) in enumerate(pieces):
        extra = 1 if n == len(pieces) - 1 else 0
        width = (share + extra) * levels
        outs = pl.pallas_call(
            functools.partial(
                adjoint_kernel, sizes=sizes, piece=(first_q, count_q, share, extra)
            ),
            grid_spec=pltpu.PrefetchScalarGridSpec(
                num_scalar_prefetch=1,
                grid=(levels,),
                in_specs=[
                    whole(members * levels, columns),
                    whole(vectors * levels, columns),
                    whole(modes, columns),
                    whole(1, columns),
                ],
                out_specs=[whole(others * width, LANES)] * inner,
                scratch_shapes=[
                    pltpu.VMEM((parts * share * levels, LANES), jnp.float32),
                    strips_shape,
                    rows_shape,
                ],
            ),
            out_shape=[jax.ShapeDtypeStruct((others * width, LANES), jnp.float32)] * inner,
            compiler_params=params,
            name=f"adjoint_{n}",
        )(where, p2, g2, horizontal, area2)
        received.append([outs[0]] + [send(outs[s], "ci", inner, s) for s in range(1, inner)])

    reduced = [
        functools.reduce(lambda a, b: a + b, blocks).reshape(others, -1, LANES)
        for blocks in received
    ]
    got = lax.all_to_all(jnp.concatenate(reduced, axis=1), everywhere, 0, 0, tiled=True)
    got = got.reshape(outer, lev, -1, levels, LANES).sum(0)
    stats = got[0, -1, 0]
    control = jnp.einsum("mal,muln->aun", vertical_all, got[:, :-1], **precise)
    squares = jnp.sum(control * control, axis=0)
    index = ci * others + rest
    place = jnp.concatenate(
        [first_q + (index * share + jnp.arange(share)) % count_q for first_q, count_q, share in pieces]
    )
    mine = (place[:, None] == jnp.arange(levels)[None, :])[:, :, None]
    squares_rows = jnp.sum(jnp.where(mine, squares[:, None, :], 0.0), axis=0)
    lifted = jnp.einsum("mal,aun->muln", vertical_all, control, **precise)
    lifted = jnp.concatenate(
        [lifted, jnp.broadcast_to(squares_rows[None, None], (lev, 1, levels, LANES))], axis=1
    ).reshape(lev, -1, LANES)
    back = jnp.broadcast_to(lifted[None], (outer,) + lifted.shape).reshape(others, -1, LANES)
    back = lax.all_to_all(back, everywhere, 0, 0, tiled=True)
    lifts = []
    begin = 0
    for n, (first_q, count_q, share) in enumerate(pieces):
        end = begin + share * levels
        if n == len(pieces) - 1:
            end += levels
        block = back[:, begin:end].reshape(-1, LANES)
        begin = end
        lifts.append([block] + [send(block, "ci", inner, s) for s in range(1, inner)])

    area_sum = stats[modes]
    factor = 1.0 / jnp.sqrt(modes * (stats[:modes] / area_sum + 1e-06))
    whole_factor = factor * (columns * inner * outer / area_sum)
    factor_rows = jnp.broadcast_to((factor * whole_factor)[:, None], (modes, columns))

    increment = None
    for n, ((first_q, count_q, share), blocks) in enumerate(zip(pieces, lifts)):
        extra = 1 if n == len(pieces) - 1 else 0
        width = (share + extra) * levels
        added = increment is not None
        increment = pl.pallas_call(
            functools.partial(
                forward_kernel, sizes=sizes, piece=(first_q, count_q, share, extra), added=added
            ),
            grid_spec=pltpu.PrefetchScalarGridSpec(
                num_scalar_prefetch=1,
                grid=(levels,),
                in_specs=[
                    whole(members * levels, columns),
                    whole(modes, columns),
                    whole(modes, columns),
                ]
                + [whole(others * width, LANES)] * inner
                + ([whole(vectors * levels, columns)] if added else []),
                out_specs=whole(vectors * levels, columns),
                scratch_shapes=[
                    pltpu.VMEM((parts * share * levels, LANES), jnp.float32),
                    strips_shape,
                    rows_shape,
                ],
            ),
            out_shape=jax.ShapeDtypeStruct((vectors * levels, columns), jnp.float32),
            compiler_params=params,
            name=f"forward_{n}",
        )(where, p2, horizontal, factor_rows, *blocks, *([increment] if added else []))

    squares_all = sum(
        jnp.sum(block.reshape(others, -1, levels, LANES)[:, -1], axis=0) for block in lifts[-1]
    )
    by_mode = squares_all[:units_a_row].reshape(modes, vectors)
    background = 0.5 * jnp.sum(by_mode * (whole_factor * whole_factor)[:, None], axis=0)
    return increment.reshape(vectors, levels, columns), background


def solution(mesh):
    count, lev = mesh.shape["col"], mesh.shape["lev"]
    inner = 4
    outer = count // inner
    split_mesh = Mesh(mesh.devices.reshape(outer, inner, lev), ("co", "ci", "lev"))
    col = ("co", "ci")
    return jax.shard_map(
        functools.partial(per_device, inner=inner, outer=outer, lev=lev),
        mesh=split_mesh,
        in_specs=(
            P(None, "lev", col),
            P(None, "lev", col),
            P(None, col),
            P(col),
            P(None, "lev"),
        ),
        out_specs=(P(None, "lev", col), P()),
        check_vma=False,
    )
```
